8 devices in a mesh: dp: 1 (over z), ep: 8 (over y, x, core).
Axes of the slice: x: 2, y: 2, z: 1, core: 2. Of those that a mesh axis runs over, the one named last changes fastest.
Arguments:
- x_in: bfloat16 [4096, 1536], P(('dp', 'ep'))
- k_cache: bfloat16 [4096, 64, 8, 64], P(('dp', 'ep'))
- v_cache: bfloat16 [4096, 64, 8, 64], P(('dp', 'ep'))
- cache_len: int32 [4096], P(('dp', 'ep'))
- topk_idx: int32 [4096, 8], P(('dp', 'ep'))
- ln_attn: bfloat16 [1536], replicated
- w_q: bfloat16 [1536, 1536], replicated
- w_k: bfloat16 [1536, 512], replicated
- w_v: bfloat16 [1536, 512], replicated
- q_norm: bfloat16 [64], replicated
- k_norm: bfloat16 [64], replicated
- w_o: bfloat16 [1536, 1536], replicated
- ln_moe: bfloat16 [1536], replicated
- w_router: bfloat16 [1536, 40], replicated
- w_gate: bfloat16 [40, 1536, 512], P('ep')
- w_up: bfloat16 [40, 1536, 512], P('ep')
- w_down: bfloat16 [40, 512, 1536], P('ep')
Outputs:
- output 1: bfloat16 [4096, 1536], P(('dp', 'ep'))
- output 2: bfloat16 [4096, 64, 8, 64], P(('dp', 'ep'))
- output 3: bfloat16 [4096, 64, 8, 64], P(('dp', 'ep'))
All inputs are finite; a program needn't handle non-finite values.
Results may differ from the reference program's by a relative error of at most 0.0144126.
Values are sent between devices in bfloat16 or wider.
A program may use at most 1 GiB of HBM per device.

```python
import jax
import jax.numpy as jnp
import numpy as np
from jax import lax

HIDDEN = 1536
Q_HEADS = 24
KV_HEADS = 8
HEAD_DIM = 64
EXPERTS = 40
TOP_K = 8
EXPERT_FF = 512
B_DEV = 512
CACHE_LEN = 64
EP_SIZE = 8
BATCH = B_DEV * EP_SIZE
E_LOCAL = EXPERTS // EP_SIZE
ROPE_BASE = 1000000.0
NORM_EPS = 1e-6


def draw_layout(len_key, route_key, local_key):
    pair_count = B_DEV * TOP_K
    cap_rows = min(B_DEV, 2 * pair_count // EP_SIZE)
    n_hot = EP_SIZE // TOP_K
    n_cold = EP_SIZE - n_hot
    rest_rows = pair_count - n_hot * cap_rows
    base_rows = rest_rows // n_cold
    extra_rows = rest_rows - base_rows * n_cold
    row_counts = [cap_rows] * n_hot + [base_rows + 1] * extra_rows + [base_rows] * (n_cold - extra_rows)
    rank_table = np.repeat(np.arange(EP_SIZE), row_counts).reshape(TOP_K, B_DEV).T
    dev_keys = jax.random.split(route_key, EP_SIZE + 1)
    dev_perm = jax.random.permutation(dev_keys[0], EP_SIZE)
    row_perms = jax.vmap(lambda key_one: jax.random.permutation(key_one, B_DEV))(dev_keys[1:])
    dev_table = dev_perm[jnp.asarray(rank_table)]
    dev_all = dev_table[row_perms]
    local_ids = jax.random.randint(local_key, (EP_SIZE, B_DEV, TOP_K), 0, E_LOCAL)
    topk_idx = (dev_all * E_LOCAL + local_ids).reshape(BATCH, TOP_K).astype(jnp.int32)
    len_keys = jax.random.split(len_key, 3)
    shard_top = jax.random.randint(len_keys[0], (EP_SIZE, 1), CACHE_LEN // 4, CACHE_LEN)
    len_draw = jax.random.randint(len_keys[1], (EP_SIZE, B_DEV), 1, shard_top).reshape(BATCH)
    longest = jax.random.randint(len_keys[2], (), 0, BATCH)
    cache_len = jnp.where(jnp.arange(BATCH) == longest, CACHE_LEN - 1, len_draw).astype(jnp.int32)
    return cache_len, topk_idx


def setup_inputs(seed: int = 0, part: int = 0) -> dict:
    base_key = jax.random.key(seed)
    part_keys = jax.random.split(jax.random.fold_in(base_key, part), 6)
    shared_keys = jax.random.split(base_key, 14)
    q_width = Q_HEADS * HEAD_DIM
    kv_width = KV_HEADS * HEAD_DIM

    def normal_of(rand_key, arr_shape, scale_mul):
        return jax.random.normal(rand_key, arr_shape, jnp.float32) * scale_mul

    cache_len, topk_idx = draw_layout(part_keys[3], part_keys[4], part_keys[5])
    cache_shape = (BATCH, CACHE_LEN, KV_HEADS, HEAD_DIM)
    return {
        'x_in': normal_of(part_keys[0], (BATCH, HIDDEN), 1.0).astype(jnp.bfloat16),
        'k_cache': normal_of(part_keys[1], cache_shape, 1.5).astype(jnp.bfloat16),
        'v_cache': normal_of(part_keys[2], cache_shape, 1.0).astype(jnp.bfloat16),
        'cache_len': cache_len,
        'topk_idx': topk_idx,
        'ln_attn': (1.0 + normal_of(shared_keys[0], (HIDDEN,), 0.3)).astype(jnp.bfloat16),
        'w_q': normal_of(shared_keys[1], (HIDDEN, q_width), HIDDEN ** -0.5).astype(jnp.bfloat16),
        'w_k': normal_of(shared_keys[2], (HIDDEN, kv_width), HIDDEN ** -0.5).astype(jnp.bfloat16),
        'w_v': normal_of(shared_keys[3], (HIDDEN, kv_width), HIDDEN ** -0.5).astype(jnp.bfloat16),
        'q_norm': (2.0 + normal_of(shared_keys[4], (HEAD_DIM,), 0.4)).astype(jnp.bfloat16),
        'k_norm': (2.0 + normal_of(shared_keys[5], (HEAD_DIM,), 0.4)).astype(jnp.bfloat16),
        'w_o': normal_of(shared_keys[6], (q_width, HIDDEN), q_width ** -0.5).astype(jnp.bfloat16),
        'ln_moe': (1.0 + normal_of(shared_keys[7], (HIDDEN,), 0.3)).astype(jnp.bfloat16),
        'w_router': normal_of(shared_keys[8], (HIDDEN, EXPERTS), 1.5 * HIDDEN ** -0.5).astype(jnp.bfloat16),
        'w_gate': normal_of(shared_keys[9], (EXPERTS, HIDDEN, EXPERT_FF), HIDDEN ** -0.5).astype(jnp.bfloat16),
        'w_up': normal_of(shared_keys[10], (EXPERTS, HIDDEN, EXPERT_FF), HIDDEN ** -0.5).astype(jnp.bfloat16),
        'w_down': normal_of(shared_keys[11], (EXPERTS, EXPERT_FF, HIDDEN), 3.0 * EXPERT_FF ** -0.5).astype(jnp.bfloat16),
    }


def norm_scale(values, gain_vec):
    return values * lax.rsqrt(jnp.mean(values * values, axis=-1, keepdims=True) + NORM_EPS) * gain_vec.astype(jnp.float32)


def rotate_halves(values, positions):
    half_dim = values.shape[-1] // 2
    freq_vec = ROPE_BASE ** (-jnp.arange(half_dim, dtype=jnp.float32) * 2.0 / values.shape[-1])
    angles = positions.astype(jnp.float32)[:, None, None] * freq_vec
    cosine = jnp.cos(angles)
    sine_val = jnp.sin(angles)
    lo_half = values[..., :half_dim]
    hi_half = values[..., half_dim:]
    return jnp.concatenate([lo_half * cosine - hi_half * sine_val, hi_half * cosine + lo_half * sine_val], axis=-1)


def reference(x_in, k_cache, v_cache, cache_len, topk_idx, ln_attn, w_q, w_k, w_v, q_norm, k_norm, w_o, ln_moe, w_router, w_gate, w_up, w_down):
    resid_in = x_in.astype(jnp.float32)
    normed = norm_scale(resid_in, ln_attn).astype(jnp.bfloat16)
    q_proj = jnp.dot(normed, w_q, preferred_element_type=jnp.float32).reshape(BATCH, Q_HEADS, HEAD_DIM)
    k_proj = jnp.dot(normed, w_k, preferred_element_type=jnp.float32).reshape(BATCH, KV_HEADS, HEAD_DIM)
    v_new = jnp.dot(normed, w_v, preferred_element_type=jnp.float32).astype(jnp.bfloat16).reshape(BATCH, KV_HEADS, HEAD_DIM)
    q_rot = rotate_halves(norm_scale(q_proj, q_norm), cache_len).astype(jnp.bfloat16)
    k_new = rotate_halves(norm_scale(k_proj, k_norm), cache_len).astype(jnp.bfloat16)
    slot_ids = jnp.arange(CACHE_LEN)
    is_new = slot_ids[None, :, None, None] == cache_len[:, None, None, None]
    k_full = jnp.where(is_new, k_new[:, None], k_cache)
    v_full = jnp.where(is_new, v_new[:, None], v_cache)

    def one_token(args_tok):
        q_tok, k_tok, v_tok, len_tok = args_tok
        q_grp = q_tok.reshape(KV_HEADS, Q_HEADS // KV_HEADS, HEAD_DIM).astype(jnp.float32)
        scores = jnp.einsum('grd,sgd->grs', q_grp, k_tok.astype(jnp.float32)) * HEAD_DIM ** -0.5
        scores = jnp.where(slot_ids <= len_tok, scores, -1e30)
        attn_prob = jax.nn.softmax(scores, axis=-1).astype(jnp.bfloat16)
        mixed = jnp.einsum('grs,sgd->grd', attn_prob.astype(jnp.float32), v_tok.astype(jnp.float32))
        return mixed.astype(jnp.bfloat16).reshape(Q_HEADS * HEAD_DIM)

    attn_out = lax.map(one_token, (q_rot, k_full, v_full, cache_len))
    x_mid = (resid_in + jnp.dot(attn_out, w_o, preferred_element_type=jnp.float32)).astype(jnp.bfloat16)
    resid_mid = x_mid.astype(jnp.float32)
    h_moe = norm_scale(resid_mid, ln_moe).astype(jnp.bfloat16)
    logits = jnp.dot(h_moe, w_router, preferred_element_type=jnp.float32)
    route_prob = jax.nn.softmax(logits, axis=-1)
    picked = jnp.take_along_axis(route_prob, topk_idx, axis=1)
    gate_wts = picked / jnp.sum(picked, axis=1, keepdims=True)
    tok_rows = jnp.repeat(h_moe, TOP_K, axis=0)

    def one_pair(args_pair):
        row_vec, expert = args_pair
        row_mat = row_vec[None, :]
        gate_act = jnp.dot(row_mat, w_gate[expert], preferred_element_type=jnp.float32)
        up_act = jnp.dot(row_mat, w_up[expert], preferred_element_type=jnp.float32)
        hidden_act = (jax.nn.silu(gate_act) * up_act).astype(jnp.bfloat16)
        return jnp.dot(hidden_act, w_down[expert], preferred_element_type=jnp.float32).astype(jnp.bfloat16)[0]

    expert_out = lax.map(one_pair, (tok_rows, topk_idx.reshape(BATCH * TOP_K)))
    moe_out = jnp.sum(expert_out.reshape(BATCH, TOP_K, HIDDEN).astype(jnp.float32) * gate_wts[:, :, None], axis=1)
    x_out = (resid_mid + moe_out).astype(jnp.bfloat16)
    return x_out, k_full, v_full
```

```python
import functools

import jax
import jax.numpy as jnp
from jax import lax
from jax.experimental import pallas as pl
from jax.experimental.pallas import tpu as pltpu
from jax.sharding import PartitionSpec as P


ROPE_BASE = 1000000.0
NORM_EPS = 1e-6
PIECE = 128
SORTED = 640
ROOM = 768


def norm_scale(values, gain_vec):
    return values * lax.rsqrt(jnp.mean(values * values, axis=-1, keepdims=True) + NORM_EPS) * gain_vec.astype(jnp.float32)


def attend_kernel(len_ref, cos_ref, sin_ref, qn_ref, kn_ref, q_ref, k_ref, v_ref, kc_ref, vc_ref, ko_ref, vo_ref, o_ref, part_ref, p_ref):
    n_rep = q_ref.shape[0]
    n_slots = kc_ref.shape[0]
    n_batch = q_ref.shape[2]
    unroll = 4

    def norm_rope(values, gain, cosine, sine):
        ms = jnp.mean(values * values, axis=0, keepdims=True)
        values = values * lax.rsqrt(ms + NORM_EPS) * gain
        half = values.shape[0] // 2
        lo, hi = values[:half], values[half:]
        return jnp.concatenate([lo * cosine - hi * sine, hi * cosine + lo * sine], axis=0).astype(jnp.bfloat16)

    for bt in range(n_batch // 128):
        lanes = pl.ds(bt * 128, 128)
        cosine, sine = cos_ref[:, lanes], sin_ref[:, lanes]
        lens = len_ref[:, lanes]
        left0 = jnp.broadcast_to(lens.astype(jnp.float32), (16, 128)).astype(jnp.bfloat16)
        k_new = norm_rope(k_ref[0, :, lanes], kn_ref[...], cosine, sine).reshape(4, 16, 128)
        v_new = v_ref[0, :, lanes].reshape(4, 16, 128)
        qs = [norm_rope(q_ref[r, :, lanes], qn_ref[...], cosine, sine).astype(jnp.float32).reshape(8, 8, 128) for r in range(n_rep)]

        def k_step(i, left):
            for u in range(unroll):
                s = i * unroll + u
                tile = jnp.where((left == 0)[None], k_new, kc_ref[s, 0, :, :, lanes])
                ko_ref[s, 0, :, :, lanes] = tile
                wide = tile.astype(jnp.float32).reshape(8, 8, 128)
                for r in range(n_rep):
                    part_ref[r, pl.ds(pl.multiple_of(s * 8, 8), 8), :] = jnp.sum(wide * qs[r], axis=0)
                left = left - jnp.ones_like(left)
            return left

        lax.fori_loop(0, n_slots // unroll, k_step, left0)
        seen = lax.broadcasted_iota(jnp.int32, (n_slots, 128), 0) <= lens
        for r in range(n_rep):
            scores = part_ref[r, pl.ds(0, n_slots, stride=8), :]
            for sub in range(1, 8):
                scores = scores + part_ref[r, pl.ds(sub, n_slots, stride=8), :]
            scores = jnp.where(seen, scores * (q_ref.shape[1] ** -0.5), -1e30)
            expd = jnp.exp(scores - jnp.max(scores, axis=0, keepdims=True))
            prob = expd / jnp.sum(expd, axis=0, keepdims=True)
            p_ref[r] = prob.astype(jnp.bfloat16).astype(jnp.float32)

        def v_step(i, carry):
            left, accs = carry
            for u in range(unroll):
                s = i * unroll + u
                tile = jnp.where((left == 0)[None], v_new, vc_ref[s, 0, :, :, lanes])
                vo_ref[s, 0, :, :, lanes] = tile
                wide = tile.astype(jnp.float32).reshape(8, 8, 128)
                accs = tuple(accs[r] + wide * p_ref[r, pl.ds(s, 1), :][None] for r in range(n_rep))
                left = left - jnp.ones_like(left)
            return left, accs

        zero = jnp.zeros((8, 8, 128), jnp.float32)
        _, accs = lax.fori_loop(0, n_slots // unroll, v_step, (left0, (zero,) * n_rep))
        for r in range(n_rep):
            o_ref[r, :, lanes] = accs[r].reshape(64, 128).astype(jnp.bfloat16)


def attend(x_in, k_cache, v_cache, cache_len, len_row, ln_attn, w_q, w_k, w_v, q_norm, k_norm):
    n_batch, n_slots, kv_heads, head_dim = k_cache.shape
    q_heads = w_q.shape[1] // head_dim
    n_rep = q_heads // kv_heads
    normed = norm_scale(x_in.astype(jnp.float32), ln_attn).astype(jnp.bfloat16)

    def proj(w):
        return jnp.dot(normed, w, preferred_element_type=jnp.float32).T.reshape(-1, head_dim, n_batch)

    q_t, k_t, v_t = proj(w_q), proj(w_k), proj(w_v).astype(jnp.bfloat16)
    half = head_dim // 2
    freq = ROPE_BASE ** (-jnp.arange(half, dtype=jnp.float32) * 2.0 / head_dim)
    angles = freq[:, None] * cache_len.astype(jnp.float32)[None, :]

    def by_slot(c):
        return c.transpose(1, 2, 3, 0).reshape(n_slots, kv_heads, 4, 16, n_batch)

    full = lambda *shape: pl.BlockSpec(shape, lambda g: (0,) * len(shape))
    cache_spec = pl.BlockSpec((n_slots, 1, 4, 16, n_batch), lambda g: (0, g, 0, 0, 0))
    head_spec = lambda n: pl.BlockSpec((n, head_dim, n_batch), lambda g: (g, 0, 0))
    cache_shape = jax.ShapeDtypeStruct((n_slots, kv_heads, 4, 16, n_batch), jnp.bfloat16)
    k_new, v_new, o_t = pl.pallas_call(
        attend_kernel,
        grid=(kv_heads,),
        in_specs=[full(1, n_batch), full(half, n_batch), full(half, n_batch), full(head_dim, 1), full(head_dim, 1),
                  head_spec(n_rep), head_spec(1), head_spec(1), cache_spec, cache_spec],
        out_specs=[cache_spec, cache_spec, head_spec(n_rep)],
        out_shape=[cache_shape, cache_shape, jax.ShapeDtypeStruct((q_heads, head_dim, n_batch), jnp.bfloat16)],
        scratch_shapes=[pltpu.VMEM((n_rep, n_slots * 8, 128), jnp.float32), pltpu.VMEM((n_rep, n_slots, 128), jnp.float32)],
        compiler_params=pltpu.CompilerParams(dimension_semantics=("arbitrary",), vmem_limit_bytes=50 * 2**20),
        cost_estimate=pl.CostEstimate(flops=50_000_000_000, bytes_accessed=140_000_000, transcendentals=0),
        name="attend",
    )(len_row[None, :], jnp.cos(angles), jnp.sin(angles), q_norm.astype(jnp.float32)[:, None], k_norm.astype(jnp.float32)[:, None],
      q_t, k_t, v_t, by_slot(k_cache), by_slot(v_cache))

    def by_row(c):
        return c.reshape(n_slots, kv_heads, head_dim, n_batch).transpose(3, 0, 1, 2)

    return o_t.reshape(q_heads * head_dim, n_batch), by_row(k_new), by_row(v_new)


def expert_kernel(n_sub, e_local, start_ref, count_ref, prow_ref, pcol_ref, r_ref, *refs):
    h_refs = refs[:2 * n_sub]
    w_refs = refs[2 * n_sub:2 * n_sub + 6]
    o_refs = refs[2 * n_sub + 6:4 * n_sub + 6]
    xs_ref, ys_ref = refs[4 * n_sub + 6:]
    step = pl.program_id(0)
    src = step // e_local
    half = h_refs[0].shape[0]
    hidden = h_refs[0].shape[1]

    @pl.when(step == 0)
    def _():
        ys_ref[...] = jnp.zeros_like(ys_ref)
        for j in range(n_sub):
            xs_ref[j, SORTED:, :] = jnp.zeros((ROOM - SORTED, hidden), jnp.bfloat16)

    @pl.when(step % e_local == 0)
    def _():
        for j in range(n_sub):
            prow = prow_ref[2 * j + src]
            for c in range(SORTED // PIECE):
                seat = lax.broadcasted_iota(jnp.int32, (PIECE, 2 * half), 0) + c * PIECE
                hot = jnp.where(seat == prow, 1.0, 0.0).astype(jnp.bfloat16)
                rows = jnp.dot(hot[:, :half], h_refs[2 * j][...], preferred_element_type=jnp.float32)
                rows = rows + jnp.dot(hot[:, half:], h_refs[2 * j + 1][...], preferred_element_type=jnp.float32)
                xs_ref[j, c * PIECE:(c + 1) * PIECE, :] = rows.astype(jnp.bfloat16)

    counts = [count_ref[j * 2 * e_local + step] for j in range(n_sub)]
    trips = functools.reduce(jnp.maximum, counts)

    def run(wg_ref, wu_ref, wd_ref):
        def piece(c, carry):
            offs = [pl.multiple_of(jnp.minimum(start_ref[j * 2 * e_local + step] + c * PIECE, SORTED), 16) for j in range(n_sub)]
            rows = jnp.concatenate([xs_ref[j, pl.ds(offs[j], PIECE), :] for j in range(n_sub)], axis=0)
            gate = jnp.dot(rows, wg_ref[0], preferred_element_type=jnp.float32)
            up = jnp.dot(rows, wu_ref[0], preferred_element_type=jnp.float32)
            act = (jax.nn.silu(gate) * up).astype(jnp.bfloat16)
            out = jnp.dot(act, wd_ref[0], preferred_element_type=jnp.float32).astype(jnp.bfloat16)
            for j in range(n_sub):
                @pl.when(c < counts[j])
                def _(j=j):
                    ys_ref[j, pl.ds(offs[j], PIECE), :] = out[j * PIECE:(j + 1) * PIECE]
            return carry

        lax.fori_loop(0, trips, piece, 0)

    def back(which, first):
        for j in range(n_sub):
            for c in range(2 * half // PIECE):
                rows = slice(c * PIECE, (c + 1) * PIECE)
                seat = lax.broadcasted_iota(jnp.int32, (PIECE, SORTED), 1)
                hot = jnp.where(seat == pcol_ref[2 * j + which, rows, :], 1.0, 0.0).astype(jnp.bfloat16)
                mine = jnp.dot(hot, ys_ref[j, :SORTED, :], preferred_element_type=jnp.float32) * r_ref[2 * j + which, rows, :]
                o_ref = o_refs[2 * j + c * PIECE // half]
                at = slice(c * PIECE % half, c * PIECE % half + PIECE)
                if first:
                    o_ref[at, :] = mine
                else:
                    o_ref[at, :] = o_ref[at, :] + mine

    @pl.when(src == 0)
    def _():
        run(*w_refs[:3])

    @pl.when(src == 1)
    def _():
        run(*w_refs[3:])

    @pl.when(step == e_local - 1)
    def _():
        back(0, True)

    @pl.when(step == 2 * e_local - 1)
    def _():
        back(1, False)


def experts(blocks, starts, counts, prow, pcol, r_col, w_own, w_par):
    n_sub = len(blocks)
    half, hidden = blocks[0][0].shape
    e_local, _, ff = w_own[0].shape
    once = pl.Buffered(1)
    full = lambda *shape: pl.BlockSpec(shape, lambda e, *_: (0,) * len(shape), pipeline_mode=once)
    own = lambda a, b: pl.BlockSpec((1, a, b), lambda e, *_: (jnp.minimum(e, e_local - 1), 0, 0))
    par = lambda a, b: pl.BlockSpec((1, a, b), lambda e, *_: (jnp.maximum(e - e_local, 0), 0, 0))
    flat = [h for block in blocks for h in block]
    out = pl.pallas_call(
        functools.partial(expert_kernel, n_sub, e_local),
        grid_spec=pltpu.PrefetchScalarGridSpec(
            num_scalar_prefetch=2,
            grid=(2 * e_local,),
            in_specs=[full(2 * n_sub, 1, 2 * half), full(2 * n_sub, 2 * half, 1), full(2 * n_sub, 2 * half, 1)]
            + [full(half, hidden)] * (2 * n_sub)
            + [own(hidden, ff), own(hidden, ff), own(ff, hidden), par(hidden, ff), par(hidden, ff), par(ff, hidden)],
            out_specs=[full(half, hidden)] * (2 * n_sub),
            scratch_shapes=[pltpu.VMEM((n_sub, ROOM, hidden), jnp.bfloat16)] * 2,
        ),
        out_shape=[jax.ShapeDtypeStruct((half, hidden), jnp.float32)] * (2 * n_sub),
        compiler_params=pltpu.CompilerParams(dimension_semantics=("arbitrary",), vmem_limit_bytes=60 * 2**20),
        cost_estimate=pl.CostEstimate(flops=n_sub * 16_000_000_000, bytes_accessed=60_000_000, transcendentals=0),
    )(starts.reshape(-1), counts.reshape(-1), prow.reshape(2 * n_sub, 1, 2 * half), pcol.reshape(2 * n_sub, 2 * half, 1), r_col.reshape(2 * n_sub, 2 * half, 1),
      *flat, *w_own, *w_par)
    return [(out[2 * j], out[2 * j + 1]) for j in range(n_sub)]


def seats(topk_blocks, me, e_local):
    n_rows = topk_blocks.shape[1]
    dev = topk_blocks // e_local
    loc = topk_blocks % e_local
    both = jnp.stack([me, me ^ 1])
    loc_src = jnp.sum(jnp.where(dev[:, None] == both[None, :, None, None], loc[:, None], 0), axis=-1)
    hot = (loc_src[:, :, None, :] == jnp.arange(e_local)[None, None, :, None])
    before = (jnp.arange(n_rows)[:, None] < jnp.arange(n_rows)[None, :]).astype(jnp.bfloat16)
    rank = lax.dot_general(hot.astype(jnp.bfloat16), before, (((3,), (0,)), ((), ())), preferred_element_type=jnp.float32).astype(jnp.int32)
    count = jnp.sum(hot.astype(jnp.int32), axis=-1)
    padded = (count + 15) // 16 * 16
    starts = [jnp.zeros_like(count[..., 0])]
    for e in range(1, e_local):
        starts.append(starts[-1] + padded[..., e - 1])
    start = jnp.stack(starts, axis=-1)
    seat = jnp.sum(jnp.where(hot, start[..., None] + rank, 0), axis=2)
    return seat, start, (count + PIECE - 1) // PIECE


def solution(mesh):
    ep_size = mesh.shape['ep']
    row_spec = P(('dp', 'ep'))
    replicated = P()
    expert_spec = P('ep')
    in_specs = (row_spec, row_spec, row_spec, row_spec, row_spec, replicated, replicated, replicated, replicated, replicated, replicated, replicated, replicated, replicated, expert_spec, expert_spec, expert_spec)
    out_specs = (row_spec, row_spec, row_spec)

    def swap(value, bit):
        return lax.ppermute(value, 'ep', [(i, i ^ bit) for i in range(ep_size)])

    def device_step(x_in, k_cache, v_cache, cache_len, topk_idx, ln_attn, w_q, w_k, w_v, q_norm, k_norm, w_o, ln_moe, w_router, w_gate, w_up, w_down):
        me = lax.axis_index('ep')
        e_local = w_gate.shape[0]
        half = x_in.shape[0] // 2
        w_own = (w_gate, w_up, w_down)
        w_par = tuple(swap(w, 1) for w in w_own)
        t_y = swap(topk_idx, 4)
        topk_blocks = jnp.stack([topk_idx, swap(topk_idx, 2), t_y, swap(t_y, 2)])
        seat, start, count = seats(topk_blocks, me, e_local)

        len_row, seat, start, count = lax.optimization_barrier((cache_len, seat, start, count))
        attn_t, k_full, v_full = attend(x_in, k_cache, v_cache, cache_len, len_row, ln_attn, w_q, w_k, w_v, q_norm, k_norm)
        resid = x_in.astype(jnp.float32)
        o_proj = lax.dot_general(attn_t, w_o, (((0,), (0,)), ((), ())), preferred_element_type=jnp.float32)
        x_mid = (resid + o_proj).astype(jnp.bfloat16)
        resid_mid = x_mid.astype(jnp.float32)
        h_moe = norm_scale(resid_mid, ln_moe).astype(jnp.bfloat16)
        h_a, h_b = h_moe[:half], h_moe[half:]

        h_xb, h_ya = swap(h_b, 2), swap(h_a, 4)
        h_xa, h_yb = swap(h_a, 2), swap(h_b, 4)
        h_da, h_db = swap(h_ya, 2), swap(h_xb, 4)

        logits = jnp.dot(h_moe, w_router, preferred_element_type=jnp.float32)
        chosen = jnp.any(topk_idx[:, :, None] == jnp.arange(logits.shape[1])[None, None, :], axis=1)
        top = jnp.max(jnp.where(chosen, logits, -jnp.inf), axis=1, keepdims=True)
        expd = jnp.where(chosen, jnp.exp(jnp.where(chosen, logits - top, 0.0)), 0.0)
        gate = expd / jnp.sum(expd, axis=1, keepdims=True)
        r_dev = jnp.sum(gate.reshape(-1, ep_size, e_local), axis=-1).T
        r_y = swap(r_dev, 4)
        r_x = swap(r_dev, 2)
        r_d = swap(r_y, 2)

        def mine(r):
            rows = lax.broadcasted_iota(jnp.int32, r.shape, 0)
            return jnp.stack([jnp.sum(jnp.where(rows == d, r, 0.0), axis=0) for d in (me, me ^ 1)])

        def call(ids, blocks, rs):
            pick = slice(ids[0], ids[-1] + 1)
            return experts(blocks, start[pick], count[pick], seat[pick], seat[pick], jnp.stack([mine(r) for r in rs]), w_own, w_par)

        (s_o,) = call((0,), [(h_a, h_b)], [r_dev])
        h_xa, h_xb, h_ya, h_yb, s_o = lax.optimization_barrier((h_xa, h_xb, h_ya, h_yb, s_o))
        s_x, s_y = call((1, 2), [(h_xa, h_xb), (h_ya, h_yb)], [r_x, r_y])
        h_da, h_db, s_x, s_y = lax.optimization_barrier((h_da, h_db, s_x, s_y))
        u_x = swap(s_x[0], 2)
        u_y = swap(s_y[1], 4)
        (s_d,) = call((3,), [(h_da, h_db)], [r_d])
        d_x, d_y = swap(s_d[0], 2), swap(s_d[1], 4)
        m_x, m_y = swap(s_x[1] + d_y, 2), swap(s_y[0] + d_x, 4)
        moe_a = s_o[0] + u_x + m_y
        moe_b = s_o[1] + u_y + m_x
        x_out = (resid_mid + jnp.concatenate([moe_a, moe_b], axis=0)).astype(jnp.bfloat16)
        return x_out, k_full, v_full

    return jax.shard_map(device_step, mesh=mesh, in_specs=in_specs, out_specs=out_specs, check_vma=False)
```

```python
import functools

import jax
import jax.numpy as jnp
from jax import lax
from jax.experimental import pallas as pl
from jax.experimental.layout import Layout, with_layout_constraint
from jax.experimental.pallas import tpu as pltpu
from jax.sharding import PartitionSpec as P


ROPE_BASE = 1000000.0
NORM_EPS = 1e-6
PIECE = 128
SORTED = 640
ROOM = 768
CHUNKS = 2


def norm_scale(values, gain_vec):
    return values * lax.rsqrt(jnp.mean(values * values, axis=-1, keepdims=True) + NORM_EPS) * gain_vec.astype(jnp.float32)


def attend_kernel(len_ref, cos_ref, sin_ref, qn_ref, kn_ref, q_ref, k_ref, v_ref, kc_ref, vc_ref, ko_ref, vo_ref, o_ref, part_ref, p_ref):
    n_rep = q_ref.shape[0]
    n_slots = kc_ref.shape[0]
    n_batch = q_ref.shape[2]
    unroll = 4

    def norm_rope(values, gain, cosine, sine):
        ms = jnp.mean(values * values, axis=0, keepdims=True)
        values = values * lax.rsqrt(ms + NORM_EPS) * gain
        half = values.shape[0] // 2
        lo, hi = values[:half], values[half:]
        return jnp.concatenate([lo * cosine - hi * sine, hi * cosine + lo * sine], axis=0).astype(jnp.bfloat16)

    for bt in range(n_batch // 128):
        lanes = pl.ds(bt * 128, 128)
        cosine, sine = cos_ref[:, lanes], sin_ref[:, lanes]
        lens = len_ref[:, lanes]
        left0 = jnp.broadcast_to(lens.astype(jnp.float32), (16, 128)).astype(jnp.bfloat16)
        k_new = norm_rope(k_ref[0, :, lanes], kn_ref[...], cosine, sine).reshape(4, 16, 128)
        v_new = v_ref[0, :, lanes].reshape(4, 16, 128)
        qs = [norm_rope(q_ref[r, :, lanes], qn_ref[...], cosine, sine).astype(jnp.float32).reshape(8, 8, 128) for r in range(n_rep)]

        def k_step(i, left):
            for u in range(unroll):
                s = i * unroll + u
                tile = jnp.where((left == 0)[None], k_new, kc_ref[s, 0, :, :, lanes])
                ko_ref[s, 0, :, :, lanes] = tile
                wide = tile.astype(jnp.float32).reshape(8, 8, 128)
                for r in range(n_rep):
                    part_ref[r, pl.ds(pl.multiple_of(s * 8, 8), 8), :] = jnp.sum(wide * qs[r], axis=0)
                left = left - jnp.ones_like(left)
            return left

        lax.fori_loop(0, n_slots // unroll, k_step, left0)
        seen = lax.broadcasted_iota(jnp.int32, (n_slots, 128), 0) <= lens
        for r in range(n_rep):
            scores = part_ref[r, pl.ds(0, n_slots, stride=8), :]
            for sub in range(1, 8):
                scores = scores + part_ref[r, pl.ds(sub, n_slots, stride=8), :]
            scores = jnp.where(seen, scores * (q_ref.shape[1] ** -0.5), -1e30)
            expd = jnp.exp(scores - jnp.max(scores, axis=0, keepdims=True))
            prob = expd / jnp.sum(expd, axis=0, keepdims=True)
            p_ref[r] = prob.astype(jnp.bfloat16).astype(jnp.float32)

        def v_step(i, carry):
            left, accs = carry
            for u in range(unroll):
                s = i * unroll + u
                tile = jnp.where((left == 0)[None], v_new, vc_ref[s, 0, :, :, lanes])
                vo_ref[s, 0, :, :, lanes] = tile
                wide = tile.astype(jnp.float32).reshape(8, 8, 128)
                accs = tuple(accs[r] + wide * p_ref[r, pl.ds(s, 1), :][None] for r in range(n_rep))
                left = left - jnp.ones_like(left)
            return left, accs

        zero = jnp.zeros((8, 8, 128), jnp.float32)
        _, accs = lax.fori_loop(0, n_slots // unroll, v_step, (left0, (zero,) * n_rep))
        for r in range(n_rep):
            o_ref[r, :, lanes] = accs[r].reshape(64, 128).astype(jnp.bfloat16)


def project(x_in, cache_len, ln_attn, w_q, w_k, w_v, head_dim):
    n_batch = x_in.shape[0]
    normed = norm_scale(x_in.astype(jnp.float32), ln_attn).astype(jnp.bfloat16)

    def proj(w):
        out = with_layout_constraint(jnp.dot(normed, w, preferred_element_type=jnp.float32), Layout(major_to_minor=(1, 0)))
        return out.T.reshape(-1, head_dim, n_batch)

    freq = ROPE_BASE ** (-jnp.arange(head_dim // 2, dtype=jnp.float32) * 2.0 / head_dim)
    angles = freq[:, None] * cache_len.astype(jnp.float32)[None, :]
    return proj(w_q), proj(w_k), proj(w_v).astype(jnp.bfloat16), jnp.cos(angles), jnp.sin(angles)


def attend(chunk, n_chunks, q_t, k_t, v_t, cosine, sine, len_row, q_gain, k_gain, k_cache, v_cache, done):
    n_slots, kv_heads, _, _, n_all = k_cache.shape
    head_dim = q_t.shape[1]
    n_batch = n_all // n_chunks
    n_rep = q_t.shape[0] // kv_heads
    full = lambda *shape: pl.BlockSpec(shape, lambda g: (0,) * len(shape))
    lane = lambda n: pl.BlockSpec((n, n_batch), lambda g: (0, chunk))
    cache_spec = pl.BlockSpec((n_slots, 1, 4, 16, n_batch), lambda g: (0, g, 0, 0, chunk))
    head_spec = lambda n: pl.BlockSpec((n, head_dim, n_batch), lambda g: (g, 0, chunk))
    out_spec = pl.BlockSpec((n_rep, head_dim, n_batch), lambda g: (g, 0, 0))
    cache_shape = jax.ShapeDtypeStruct(k_cache.shape, jnp.bfloat16)
    n_done = len(done)

    def body(*refs):
        attend_kernel(*refs[n_done:])

    return pl.pallas_call(
        body,
        grid=(kv_heads,),
        in_specs=[pl.BlockSpec(memory_space=pl.ANY)] * n_done + [lane(1), lane(head_dim // 2), lane(head_dim // 2), full(head_dim, 1), full(head_dim, 1),
                  head_spec(n_rep), head_spec(1), head_spec(1), cache_spec, cache_spec],
        out_specs=[cache_spec, cache_spec, out_spec],
        out_shape=[cache_shape, cache_shape, jax.ShapeDtypeStruct((q_t.shape[0], head_dim, n_batch), jnp.bfloat16)],
        input_output_aliases={i: i for i in range(n_done)},
        scratch_shapes=[pltpu.VMEM((n_rep, n_slots * 8, 128), jnp.float32), pltpu.VMEM((n_rep, n_slots, 128), jnp.float32)],
        compiler_params=pltpu.CompilerParams(dimension_semantics=("arbitrary",), vmem_limit_bytes=40 * 2**20),
        cost_estimate=pl.CostEstimate(flops=30_000_000_000, bytes_accessed=70_000_000, transcendentals=0),
        name="attend",
    )(*done, len_row, cosine, sine, q_gain, k_gain, q_t, k_t, v_t, k_cache, v_cache)


def expert_kernel(n_sub, e_local, dev_ref, start_ref, count_ref, prow_ref, *refs):
    r_refs = refs[:2 * n_sub]
    h_refs = refs[2 * n_sub:4 * n_sub]
    w_refs = refs[4 * n_sub:4 * n_sub + 6]
    o_refs = refs[4 * n_sub + 6:8 * n_sub + 6]
    xs_ref, ys_ref, wg_ref, wu_ref, wd_ref, sem = refs[8 * n_sub + 6:]
    bufs = (wg_ref, wu_ref, wd_ref)
    ring = wg_ref.shape[0]
    step = pl.program_id(0)
    steps = 2 * e_local
    src = step // e_local
    half, hidden = h_refs[0].shape

    def copy(e, k, first):
        source = w_refs[k].at[e] if first else w_refs[3 + k].at[e - e_local]
        return pltpu.make_async_copy(source, bufs[k].at[lax.rem(e, ring)], sem.at[lax.rem(e, ring), k])

    def fetch(e):
        for first in (True, False):
            @pl.when((e < e_local) if first else ((e >= e_local) & (e < steps)))
            def _(first=first):
                for k in range(3):
                    copy(e, k, first).start()

    @pl.when(step == 0)
    def _():
        for e in range(ring - 1):
            fetch(jnp.int32(e))
        ys_ref[...] = jnp.zeros_like(ys_ref)
        for j in range(n_sub):
            xs_ref[j, SORTED:, :] = jnp.zeros((ROOM - SORTED, hidden), jnp.bfloat16)

    fetch(step + ring - 1)

    @pl.when(step % e_local == 0)
    def _():
        for j in range(n_sub):
            prow = prow_ref[pl.ds(2 * j + src, 1), :]
            for c in range(SORTED // PIECE):
                seat = lax.broadcasted_iota(jnp.int32, (PIECE, 2 * half), 0) + c * PIECE
                hot = jnp.where(seat == prow, 1.0, 0.0).astype(jnp.bfloat16)
                rows = jnp.dot(hot[:, :half], h_refs[2 * j][...], preferred_element_type=jnp.float32)
                rows = rows + jnp.dot(hot[:, half:], h_refs[2 * j + 1][...], preferred_element_type=jnp.float32)
                xs_ref[j, c * PIECE:(c + 1) * PIECE, :] = rows.astype(jnp.bfloat16)

    slot = lax.rem(step, ring)
    for k in range(3):
        pltpu.make_async_copy(w_refs[k].at[0], bufs[k].at[slot], sem.at[slot, k]).wait()
    counts = [count_ref[j * steps + step] for j in range(n_sub)]

    def piece(c, carry):
        offs = [pl.multiple_of(jnp.minimum(start_ref[j * steps + step] + c * PIECE, SORTED), 16) for j in range(n_sub)]
        rows = jnp.concatenate([xs_ref[j, pl.ds(offs[j], PIECE), :] for j in range(n_sub)], axis=0)
        gate = jnp.dot(rows, wg_ref[slot], preferred_element_type=jnp.float32)
        up = jnp.dot(rows, wu_ref[slot], preferred_element_type=jnp.float32)
        act = (jax.nn.silu(gate) * up).astype(jnp.bfloat16)
        out = jnp.dot(act, wd_ref[slot], preferred_element_type=jnp.float32).astype(jnp.bfloat16)
        for j in range(n_sub):
            @pl.when(c < counts[j])
            def _(j=j):
                ys_ref[j, pl.ds(offs[j], PIECE), :] = out[j * PIECE:(j + 1) * PIECE]
        return carry

    lax.fori_loop(0, functools.reduce(jnp.maximum, counts), piece, 0)

    def column(row):
        return jnp.broadcast_to(row, (128, row.shape[1])).T

    def back(which):
        dev = dev_ref[which]
        for j in range(n_sub):
            seat_col = column(prow_ref[pl.ds(2 * j + which, 1), :].astype(jnp.float32))
            for i in range(2):
                r_col = column(r_refs[2 * j + i][pl.ds(dev, 1), :])
                for c in range(half // PIECE):
                    at = seat_col[i * half + c * PIECE:i * half + (c + 1) * PIECE]
                    lane = lax.broadcasted_iota(jnp.int32, (PIECE, 128), 1).astype(jnp.float32)
                    hot = jnp.concatenate([jnp.where(at == lane + t * 128.0, 1.0, 0.0).astype(jnp.bfloat16) for t in range(SORTED // 128)], axis=1)
                    r_rows = r_col[c * PIECE:(c + 1) * PIECE]
                    mine = jnp.dot(hot, ys_ref[j, :SORTED, :], preferred_element_type=jnp.float32) * jnp.concatenate([r_rows] * (hidden // 128), axis=1)
                    o_ref = o_refs[4 * j + 2 * i + c]
                    o_ref[...] = mine if which == 0 else o_ref[...] + mine

    @pl.when(step == e_local - 1)
    def _():
        back(0)

    @pl.when(step == steps - 1)
    def _():
        back(1)


def experts(blocks, r_blocks, devs, starts, counts, seat, w_own, w_par):
    n_sub = len(blocks) // 2
    half, hidden = blocks[0].shape
    e_local, _, ff = w_own[0].shape
    ring = 4
    once = pl.Buffered(1)
    full = lambda *shape: pl.BlockSpec(shape, lambda e, *_: (0,) * len(shape), pipeline_mode=once)
    out = pl.pallas_call(
        functools.partial(expert_kernel, n_sub, e_local),
        grid_spec=pltpu.PrefetchScalarGridSpec(
            num_scalar_prefetch=3,
            grid=(2 * e_local,),
            in_specs=[full(2 * n_sub, 2 * half)] + [full(*r.shape) for r in r_blocks] + [full(half, hidden)] * (2 * n_sub)
            + [pl.BlockSpec(memory_space=pl.ANY)] * 6,
            out_specs=[full(PIECE, hidden)] * (4 * n_sub),
            scratch_shapes=[pltpu.VMEM((n_sub, ROOM, hidden), jnp.bfloat16)] * 2
            + [pltpu.VMEM((ring, hidden, ff), jnp.bfloat16)] * 2 + [pltpu.VMEM((ring, ff, hidden), jnp.bfloat16), pltpu.SemaphoreType.DMA((ring, 3))],
        ),
        out_shape=[jax.ShapeDtypeStruct((PIECE, hidden), jnp.float32)] * (4 * n_sub),
        compiler_params=pltpu.CompilerParams(dimension_semantics=("arbitrary",), vmem_limit_bytes=58 * 2**20),
        cost_estimate=pl.CostEstimate(flops=n_sub * 16_000_000_000, bytes_accessed=60_000_000, transcendentals=0),
        name="experts",
    )(devs, starts.reshape(-1), counts.reshape(-1), seat.reshape(2 * n_sub, 2 * half), *r_blocks, *blocks, *w_own, *w_par)
    return [(out[2 * i], out[2 * i + 1]) for i in range(2 * n_sub)]


def seats(topk_blocks, me, e_local):
    n_rows = topk_blocks.shape[1]
    dev = topk_blocks // e_local
    loc = topk_blocks % e_local
    both = jnp.stack([me, me ^ 1])
    loc_src = jnp.sum(jnp.where(dev[:, None] == both[None, :, None, None], loc[:, None], 0), axis=-1)
    hot = (loc_src[:, :, None, :] == jnp.arange(e_local)[None, None, :, None])
    before = (jnp.arange(n_rows)[:, None] < jnp.arange(n_rows)[None, :]).astype(jnp.bfloat16)
    rank = lax.dot_general(hot.astype(jnp.bfloat16), before, (((3,), (0,)), ((), ())), preferred_element_type=jnp.float32).astype(jnp.int32)
    count = jnp.sum(hot.astype(jnp.int32), axis=-1)
    padded = (count + 15) // 16 * 16
    starts = [jnp.zeros_like(count[..., 0])]
    for e in range(1, e_local):
        starts.append(starts[-1] + padded[..., e - 1])
    start = jnp.stack(starts, axis=-1)
    seat = jnp.sum(jnp.where(hot, start[..., None] + rank, 0), axis=2)
    return seat, start, (count + PIECE - 1) // PIECE


def solution(mesh):
    ep_size = mesh.shape['ep']
    row_spec = P(('dp', 'ep'))
    replicated = P()
    expert_spec = P('ep')
    in_specs = (row_spec, row_spec, row_spec, row_spec, row_spec, replicated, replicated, replicated, replicated, replicated, replicated, replicated, replicated, replicated, expert_spec, expert_spec, expert_spec)
    out_specs = (row_spec, row_spec, row_spec)

    def swap(value, bit):
        return lax.ppermute(value, 'ep', [(i, i ^ bit) for i in range(ep_size)])

    def device_step(x_in, k_cache, v_cache, cache_len, topk_idx, ln_attn, w_q, w_k, w_v, q_norm, k_norm, w_o, ln_moe, w_router, w_gate, w_up, w_down):
        me = lax.axis_index('ep')
        e_local = w_gate.shape[0]
        n_batch, n_slots, kv_heads, head_dim = k_cache.shape
        n_rows = n_batch // CHUNKS
        top_k = topk_idx.shape[1]
        w_own = (w_gate, w_up, w_down)
        w_par = tuple(swap(w, 1) for w in w_own)
        blocks = jnp.stack([topk_idx, swap(topk_idx, 2), swap(topk_idx, 4), swap(topk_idx, 6)])
        blocks = blocks.reshape(2, 2, CHUNKS, n_rows, top_k).transpose(2, 0, 1, 3, 4).reshape(2 * CHUNKS, 2 * n_rows, top_k)
        seat, start, count = seats(blocks, me, e_local)
        devs = jnp.stack([me, me ^ 1]).astype(jnp.int32)

        q_t, k_t, v_t, cosine, sine = project(x_in, cache_len, ln_attn, w_q, w_k, w_v, head_dim)
        by_slot = lambda c: c.transpose(1, 2, 3, 0).reshape(n_slots, kv_heads, 4, 16, n_batch)
        k_slots, v_slots = by_slot(k_cache), by_slot(v_cache)
        gains = (q_norm.astype(jnp.float32)[:, None], k_norm.astype(jnp.float32)[:, None])
        len_row, seat, start, count = lax.optimization_barrier((cache_len[None, :], seat, start, count))

        done, resid, own, far, gates = (), [], [], [], []
        for c in range(CHUNKS):
            if c:
                len_row, own[c - 1] = lax.optimization_barrier((len_row, own[c - 1]))
            k_full, v_full, attn_t = attend(c, CHUNKS, q_t, k_t, v_t, cosine, sine, len_row, *gains, k_slots, v_slots, done)
            done = (k_full, v_full)
            rows = slice(c * n_rows, (c + 1) * n_rows)
            o_proj = lax.dot_general(attn_t.reshape(-1, n_rows), w_o, (((0,), (0,)), ((), ())), preferred_element_type=jnp.float32)
            x_mid = (x_in[rows].astype(jnp.float32) + o_proj).astype(jnp.bfloat16)
            resid.append(x_mid.astype(jnp.float32))
            h_moe = norm_scale(resid[c], ln_moe).astype(jnp.bfloat16)
            own.append(h_moe)
            h_x = swap(h_moe, 2)
            h_y = swap(h_moe, 4)
            h_d = swap(h_moe, 6)
            far.append((h_x, h_y, h_d))

            logits = jnp.dot(h_moe, w_router, preferred_element_type=jnp.float32)
            chosen = jnp.any(topk_idx[rows][:, :, None] == jnp.arange(logits.shape[1])[None, None, :], axis=1)
            top = jnp.max(jnp.where(chosen, logits, -jnp.inf), axis=1, keepdims=True)
            expd = jnp.where(chosen, jnp.exp(jnp.where(chosen, logits - top, 0.0)), 0.0)
            gate = expd / jnp.sum(expd, axis=1, keepdims=True)
            r_dev = jnp.sum(gate.reshape(-1, ep_size, e_local), axis=-1).T
            gates.append((r_dev, swap(r_dev, 2), swap(r_dev, 4), swap(r_dev, 6)))

        sums = []
        for c in range(CHUNKS):
            h_o, h_far = own[c], far[c]
            if c == 0:
                h_o, own[-1] = lax.optimization_barrier((h_o, own[-1]))
            else:
                h_far, sums[c - 1] = lax.optimization_barrier((h_far, sums[c - 1]))
            pick = slice(2 * c, 2 * c + 2)
            s_o, s_x, s_y, s_d = experts([h_o, *h_far], gates[c], devs, start[pick], count[pick], seat[pick], w_own, w_par)
            sums.append((s_o, s_x, s_y, s_d))
        outs = []
        sent = []
        for c in range(CHUNKS):
            s_o, s_x, s_y, s_d = sums[c]
            d_x = swap(s_d[0], 2)
            d_y = swap(s_d[1], 4)
            u_x = swap(s_x[0], 2)
            u_y = swap(s_y[1], 4)
            sent.append((d_x, d_y, u_x, u_y))
        last = sums[-1][0][0]
        for c in range(CHUNKS):
            s_o, s_x, s_y, s_d = sums[c]
            d_x, d_y, u_x, u_y = sent[c]
            if c < CHUNKS - 1:
                d_x, d_y, last = lax.optimization_barrier((d_x, d_y, last))
                sums[-1] = ((last, sums[-1][0][1]), *sums[-1][1:])
            m_x, m_y = swap(s_x[1] + d_y, 2), swap(s_y[0] + d_x, 4)
            outs += [s_o[0] + u_x + m_y, s_o[1] + u_y + m_x]
        x_out = (jnp.concatenate(resid, axis=0) + jnp.concatenate(outs, axis=0)).astype(jnp.bfloat16)
        by_row = lambda c: c.reshape(n_slots, kv_heads, head_dim, n_batch).transpose(3, 0, 1, 2)
        return x_out, by_row(k_full), by_row(v_full)

    return jax.shard_map(device_step, mesh=mesh, in_specs=in_specs, out_specs=out_specs, check_vma=False)
```

```python
import functools

import jax
import jax.numpy as jnp
from jax import lax
from jax.experimental import pallas as pl
from jax.experimental.layout import Layout, with_layout_constraint
from jax.experimental.pallas import tpu as pltpu
from jax.sharding import PartitionSpec as P


ROPE_BASE = 1000000.0
NORM_EPS = 1e-6
PIECE = 128
SORTED = 640
ROOM = 768
CHUNKS = 2


def norm_scale(values, gain_vec):
    return values * lax.rsqrt(jnp.mean(values * values, axis=-1, keepdims=True) + NORM_EPS) * gain_vec.astype(jnp.float32)


def attend_kernel(len_ref, cos_ref, sin_ref, qn_ref, kn_ref, q_ref, k_ref, v_ref, kc_ref, vc_ref, ko_ref, vo_ref, o_ref, part_ref, p_ref):
    n_rep = q_ref.shape[0]
    n_slots = kc_ref.shape[0]
    n_batch = q_ref.shape[2]
    unroll = 16

    def norm_rope(values, gain, cosine, sine):
        ms = jnp.mean(values * values, axis=0, keepdims=True)
        values = values * lax.rsqrt(ms + NORM_EPS) * gain
        half = values.shape[0] // 2
        lo, hi = values[:half], values[half:]
        return jnp.concatenate([lo * cosine - hi * sine, hi * cosine + lo * sine], axis=0).astype(jnp.bfloat16)

    for bt in range(n_batch // 128):
        lanes = pl.ds(bt * 128, 128)
        cosine, sine = cos_ref[:, lanes], sin_ref[:, lanes]
        lens = len_ref[:, lanes]
        left0 = jnp.broadcast_to(lens.astype(jnp.float32), (8, 128)).astype(jnp.bfloat16)
        k_new = norm_rope(k_ref[0, :, lanes], kn_ref[...], cosine, sine).reshape(8, 8, 128)
        v_new = v_ref[0, :, lanes].reshape(8, 8, 128)
        qs = [norm_rope(q_ref[r, :, lanes], qn_ref[...], cosine, sine).astype(jnp.float32).reshape(8, 8, 128) for r in range(n_rep)]

        def k_step(i, left):
            for u in range(unroll):
                s = i * unroll + u
                here = left == 0
                sums = [None] * n_rep
                for t in range(8):
                    tile = jnp.where(here, k_new[t], kc_ref[s, 0, t, :, lanes])
                    ko_ref[s, 0, t, :, lanes] = tile
                    wide = tile.astype(jnp.float32)
                    for v in range(1):
                        for r in range(n_rep):
                            term = wide[8 * v:8 * v + 8] * qs[r][1 * t + v]
                            sums[r] = term if sums[r] is None else sums[r] + term
                for r in range(n_rep):
                    part_ref[r, pl.ds(pl.multiple_of(s * 8, 8), 8), :] = sums[r]
                left = left - jnp.ones_like(left)
            return left

        lax.fori_loop(0, n_slots // unroll, k_step, left0)
        seen = lax.broadcasted_iota(jnp.int32, (n_slots, 128), 0) <= lens
        for r in range(n_rep):
            scores = part_ref[r, pl.ds(0, n_slots, stride=8), :]
            for sub in range(1, 8):
                scores = scores + part_ref[r, pl.ds(sub, n_slots, stride=8), :]
            scores = jnp.where(seen, scores * (q_ref.shape[1] ** -0.5), -1e30)
            expd = jnp.exp(scores - jnp.max(scores, axis=0, keepdims=True))
            prob = expd / jnp.sum(expd, axis=0, keepdims=True)
            p_ref[r] = prob.astype(jnp.bfloat16).astype(jnp.float32)

        def v_step(i, carry):
            left, accs = carry
            for u in range(unroll):
                s = i * unroll + u
                here = left == 0
                probs = [jnp.broadcast_to(p_ref[r, pl.ds(s, 1), :], (8, 128)) for r in range(n_rep)]
                accs = list(accs)
                for t in range(8):
                    tile = jnp.where(here, v_new[t], vc_ref[s, 0, t, :, lanes])
                    vo_ref[s, 0, t, :, lanes] = tile
                    wide = tile.astype(jnp.float32)
                    for v in range(1):
                        for r in range(n_rep):
                            at = 8 * r + 1 * t + v
                            accs[at] = accs[at] + wide[8 * v:8 * v + 8] * probs[r]
                accs = tuple(accs)
                left = left - jnp.ones_like(left)
            return left, accs

        zero = jnp.zeros((8, 128), jnp.float32)
        _, accs = lax.fori_loop(0, n_slots // unroll, v_step, (left0, (zero,) * (8 * n_rep)))
        for r in range(n_rep):
            o_ref[r, :, lanes] = jnp.concatenate(accs[8 * r:8 * r + 8], axis=0).astype(jnp.bfloat16)


def project(x_in, cache_len, ln_attn, w_q, w_k, w_v, head_dim):
    n_batch = x_in.shape[0]
    normed = norm_scale(x_in.astype(jnp.float32), ln_attn).astype(jnp.bfloat16)

    def proj(w):
        out = with_layout_constraint(jnp.dot(normed, w, preferred_element_type=jnp.float32), Layout(major_to_minor=(1, 0)))
        return out.T.reshape(-1, head_dim, n_batch)

    freq = ROPE_BASE ** (-jnp.arange(head_dim // 2, dtype=jnp.float32) * 2.0 / head_dim)
    angles = freq[:, None] * cache_len.astype(jnp.float32)[None, :]
    return proj(w_q), proj(w_k), proj(w_v).astype(jnp.bfloat16), jnp.cos(angles), jnp.sin(angles)


def attend(chunk, n_chunks, q_t, k_t, v_t, cosine, sine, len_row, q_gain, k_gain, k_cache, v_cache, done):
    n_slots, kv_heads, _, _, n_all = k_cache.shape
    head_dim = q_t.shape[1]
    n_batch = n_all // n_chunks
    n_rep = q_t.shape[0] // kv_heads
    full = lambda *shape: pl.BlockSpec(shape, lambda g: (0,) * len(shape))
    lane = lambda n: pl.BlockSpec((n, n_batch), lambda g: (0, chunk))
    cache_spec = pl.BlockSpec((n_slots, 1, 8, 8, n_batch), lambda g: (0, g, 0, 0, chunk))
    head_spec = lambda n: pl.BlockSpec((n, head_dim, n_batch), lambda g: (g, 0, chunk))
    out_spec = pl.BlockSpec((n_rep, head_dim, n_batch), lambda g: (g, 0, 0))
    cache_shape = jax.ShapeDtypeStruct(k_cache.shape, jnp.bfloat16)
    n_done = len(done)

    def body(*refs):
        attend_kernel(*refs[n_done:])

    return pl.pallas_call(
        body,
        grid=(kv_heads,),
        in_specs=[pl.BlockSpec(memory_space=pl.ANY)] * n_done + [lane(1), lane(head_dim // 2), lane(head_dim // 2), full(head_dim, 1), full(head_dim, 1),
                  head_spec(n_rep), head_spec(1), head_spec(1), cache_spec, cache_spec],
        out_specs=[cache_spec, cache_spec, out_spec],
        out_shape=[cache_shape, cache_shape, jax.ShapeDtypeStruct((q_t.shape[0], head_dim, n_batch), jnp.bfloat16)],
        input_output_aliases={i: i for i in range(n_done)},
        scratch_shapes=[pltpu.VMEM((n_rep, n_slots * 8, 128), jnp.float32), pltpu.VMEM((n_rep, n_slots, 128), jnp.float32)],
        compiler_params=pltpu.CompilerParams(dimension_semantics=("arbitrary",), vmem_limit_bytes=40 * 2**20),
        cost_estimate=pl.CostEstimate(flops=30_000_000_000, bytes_accessed=70_000_000, transcendentals=0),
        name="attend",
    )(*done, len_row, cosine, sine, q_gain, k_gain, q_t, k_t, v_t, k_cache, v_cache)


def expert_kernel(n_sub, e_local, dev_ref, wr_ref, *refs):
    t_refs = refs[:2 * n_sub]
    h_refs = refs[2 * n_sub:4 * n_sub]
    w_refs = refs[4 * n_sub:4 * n_sub + 6]
    o_refs = refs[4 * n_sub + 6:8 * n_sub + 6]
    xs_ref, ys_ref, wg_ref, wu_ref, wd_ref, prow_ref, r_ref, number_ref, number_smem, sem, number_sem = refs[8 * n_sub + 6:]
    bufs = (wg_ref, wu_ref, wd_ref)
    ring = wg_ref.shape[0]
    step = pl.program_id(0)
    steps = 2 * e_local
    src = step // e_local
    half, hidden = h_refs[0].shape

    def copy(e, k, first):
        source = w_refs[k].at[e] if first else w_refs[3 + k].at[e - e_local]
        return pltpu.make_async_copy(source, bufs[k].at[lax.rem(e, ring)], sem.at[lax.rem(e, ring), k])

    def fetch(e):
        for first in (True, False):
            @pl.when((e < e_local) if first else ((e >= e_local) & (e < steps)))
            def _(first=first):
                for k in range(3):
                    copy(e, k, first).start()

    @pl.when(step == 0)
    def _():
        for e in range(ring - 1):
            fetch(jnp.int32(e))
        ys_ref[...] = jnp.zeros_like(ys_ref)
        for j in range(n_sub):
            xs_ref[j, SORTED:, :] = jnp.zeros((ROOM - SORTED, hidden), jnp.bfloat16)

        locals_of = {}
        for q in range(2 * n_sub):
            picks = t_refs[q][...]
            n_experts = wr_ref.shape[0]
            logits = lax.dot_general(wr_ref[...], h_refs[q][...], (((1,), (1,)), ((), ())), preferred_element_type=jnp.float32)
            expert = lax.broadcasted_iota(jnp.int32, (n_experts, half), 0)
            times = jnp.zeros((n_experts, half), jnp.float32)
            for k in range(picks.shape[0]):
                times = times + jnp.where(expert == picks[k:k + 1], 1.0, 0.0)
            chosen = times > 0.0
            top = jnp.max(jnp.where(chosen, logits, -3.4e38), axis=0, keepdims=True)
            expd = jnp.where(chosen, jnp.exp(jnp.where(chosen, logits - top, 0.0)), 0.0)
            gate = expd / jnp.sum(expd, axis=0, keepdims=True)
            for which in range(2):
                low = dev_ref[which] * e_local
                r_ref[2 * q + which:2 * q + which + 1, :] = jnp.sum(jnp.where((expert >= low) & (expert < low + e_local), gate, 0.0), axis=0, keepdims=True)
                here = (picks >= low) & (picks < low + e_local)
                locals_of[q, which] = jnp.sum(jnp.where(here, (picks - low).astype(jnp.float32), 0.0), axis=0, keepdims=True)
        lane_a = lax.broadcasted_iota(jnp.int32, (2 * half, 2 * half), 0)
        lane_b = lax.broadcasted_iota(jnp.int32, (2 * half, 2 * half), 1)
        before = jnp.where(lane_a < lane_b, 1.0, 0.0).astype(jnp.bfloat16)
        local = lax.broadcasted_iota(jnp.int32, (16, 2 * half), 0).astype(jnp.float32)
        for j in range(n_sub):
            for which in range(2):
                loc = jnp.concatenate([locals_of[2 * j, which], locals_of[2 * j + 1, which]], axis=1)
                hot = jnp.where(local == loc, 1.0, 0.0)
                rank = jnp.dot(hot.astype(jnp.bfloat16), before, preferred_element_type=jnp.float32)
                number = jnp.sum(hot, axis=1, keepdims=True)
                padded = ((number.astype(jnp.int32) + 15) // 16 * 16).astype(jnp.float32)
                first = jnp.zeros((1, 1), jnp.float32)
                seat = jnp.zeros((1, 2 * half), jnp.float32)
                for e in range(e_local):
                    seat = seat + hot[e:e + 1] * (rank[e:e + 1] + first)
                    first = first + padded[e:e + 1]
                prow_ref[2 * j + which:2 * j + which + 1, :] = seat.astype(jnp.int32)
                number_ref[2 * j + which] = jnp.broadcast_to(number[:8], (8, 128)).astype(jnp.int32)

    fetch(step + ring - 1)

    @pl.when(step % e_local == 0)
    def _():
        for j in range(n_sub):
            prow = prow_ref[pl.ds(2 * j + src, 1), :]
            for c in range(SORTED // PIECE):
                seat = lax.broadcasted_iota(jnp.int32, (PIECE, 2 * half), 0) + c * PIECE
                hot = jnp.where(seat == prow, 1.0, 0.0).astype(jnp.bfloat16)
                rows = jnp.dot(hot[:, :half], h_refs[2 * j][...], preferred_element_type=jnp.float32)
                rows = rows + jnp.dot(hot[:, half:], h_refs[2 * j + 1][...], preferred_element_type=jnp.float32)
                xs_ref[j, c * PIECE:(c + 1) * PIECE, :] = rows.astype(jnp.bfloat16)

    @pl.when(step == 0)
    def _():
        to_scalars = pltpu.make_async_copy(number_ref, number_smem, number_sem)
        to_scalars.start()
        to_scalars.wait()

    slot = lax.rem(step, ring)
    for k in range(3):
        pltpu.make_async_copy(w_refs[k].at[0], bufs[k].at[slot], sem.at[slot, k]).wait()
    mine_e = step - src * e_local
    counts, starts = [], []
    for j in range(n_sub):
        counts.append((number_smem[2 * j + src, mine_e, 0] + PIECE - 1) // PIECE)
        first = jnp.int32(0)
        for e in range(e_local - 1):
            first = first + jnp.where(e < mine_e, (number_smem[2 * j + src, e, 0] + 15) // 16 * 16, 0)
        starts.append(first)

    def piece(c, carry):
        offs = [pl.multiple_of(jnp.minimum(starts[j] + c * PIECE, SORTED), 16) for j in range(n_sub)]
        rows = jnp.concatenate([xs_ref[j, pl.ds(offs[j], PIECE), :] for j in range(n_sub)], axis=0)
        gate = jnp.dot(rows, wg_ref[slot], preferred_element_type=jnp.float32)
        up = jnp.dot(rows, wu_ref[slot], preferred_element_type=jnp.float32)
        act = (jax.nn.silu(gate) * up).astype(jnp.bfloat16)
        out = jnp.dot(act, wd_ref[slot], preferred_element_type=jnp.float32).astype(jnp.bfloat16)
        for j in range(n_sub):
            @pl.when(c < counts[j])
            def _(j=j):
                ys_ref[j, pl.ds(offs[j], PIECE), :] = out[j * PIECE:(j + 1) * PIECE]
        return carry

    lax.fori_loop(0, functools.reduce(jnp.maximum, counts), piece, 0)

    def column(row):
        return jnp.broadcast_to(row, (128, row.shape[1])).T

    def back(which):
        for j in range(n_sub):
            seat_col = column(prow_ref[2 * j + which:2 * j + which + 1, :].astype(jnp.float32))
            for i in range(2):
                r_col = column(r_ref[2 * (2 * j + i) + which:2 * (2 * j + i) + which + 1, :])
                for c in range(half // PIECE):
                    at = seat_col[i * half + c * PIECE:i * half + (c + 1) * PIECE]
                    lane = lax.broadcasted_iota(jnp.int32, (PIECE, 128), 1).astype(jnp.float32)
                    hot = jnp.concatenate([jnp.where(at == lane + t * 128.0, 1.0, 0.0).astype(jnp.bfloat16) for t in range(SORTED // 128)], axis=1)
                    r_rows = r_col[c * PIECE:(c + 1) * PIECE]
                    mine = jnp.dot(hot, ys_ref[j, :SORTED, :], preferred_element_type=jnp.float32) * jnp.concatenate([r_rows] * (hidden // 128), axis=1)
                    o_ref = o_refs[4 * j + 2 * i + c]
                    o_ref[...] = mine if which == 0 else o_ref[...] + mine

    @pl.when(step == e_local - 1)
    def _():
        back(0)

    @pl.when(step == steps - 1)
    def _():
        back(1)


def experts(chunk, blocks, t_blocks, devs, w_r, w_own, w_par):
    n_sub = len(blocks) // 2
    half, hidden = blocks[0].shape
    e_local, _, ff = w_own[0].shape
    ring = 4
    once = pl.Buffered(1)
    full = lambda *shape: pl.BlockSpec(shape, lambda e, *_: (0,) * len(shape), pipeline_mode=once)
    out = pl.pallas_call(
        functools.partial(expert_kernel, n_sub, e_local),
        grid_spec=pltpu.PrefetchScalarGridSpec(
            num_scalar_prefetch=1,
            grid=(2 * e_local,),
            in_specs=[full(*w_r.shape)] + [pl.BlockSpec((t_blocks[0].shape[0], half), lambda e, *_: (0, chunk))] * (2 * n_sub) + [full(half, hidden)] * (2 * n_sub)
            + [pl.BlockSpec(memory_space=pl.ANY)] * 6,
            out_specs=[full(PIECE, hidden)] * (4 * n_sub),
            scratch_shapes=[pltpu.VMEM((n_sub, ROOM, hidden), jnp.bfloat16)] * 2
            + [pltpu.VMEM((ring, hidden, ff), jnp.bfloat16)] * 2 + [pltpu.VMEM((ring, ff, hidden), jnp.bfloat16)]
            + [pltpu.VMEM((2 * n_sub, 2 * half), jnp.int32), pltpu.VMEM((4 * n_sub, half), jnp.float32), pltpu.VMEM((2 * n_sub, 8, 128), jnp.int32),
               pltpu.SMEM((2 * n_sub, 8, 128), jnp.int32), pltpu.SemaphoreType.DMA((ring, 3)), pltpu.SemaphoreType.DMA],
        ),
        out_shape=[jax.ShapeDtypeStruct((PIECE, hidden), jnp.float32)] * (4 * n_sub),
        compiler_params=pltpu.CompilerParams(dimension_semantics=("arbitrary",), vmem_limit_bytes=58 * 2**20),
        cost_estimate=pl.CostEstimate(flops=n_sub * 16_000_000_000, bytes_accessed=60_000_000, transcendentals=0),
        name="experts",
    )(devs, w_r, *t_blocks, *blocks, *w_own, *w_par)
    return [(out[2 * i], out[2 * i + 1]) for i in range(2 * n_sub)]


def solution(mesh):
    ep_size = mesh.shape['ep']
    row_spec = P(('dp', 'ep'))
    replicated = P()
    expert_spec = P('ep')
    in_specs = (row_spec, row_spec, row_spec, row_spec, row_spec, replicated, replicated, replicated, replicated, replicated, replicated, replicated, replicated, replicated, expert_spec, expert_spec, expert_spec)
    out_specs = (row_spec, row_spec, row_spec)

    def swap(value, bit):
        return lax.ppermute(value, 'ep', [(i, i ^ bit) for i in range(ep_size)])

    def device_step(x_in, k_cache, v_cache, cache_len, topk_idx, ln_attn, w_q, w_k, w_v, q_norm, k_norm, w_o, ln_moe, w_router, w_gate, w_up, w_down):
        me = lax.axis_index('ep')
        n_batch, n_slots, kv_heads, head_dim = k_cache.shape
        n_rows = n_batch // CHUNKS
        w_own = (w_gate, w_up, w_down)
        w_par = tuple(swap(w, 1) for w in w_own)
        devs = jnp.stack([me, me ^ 1]).astype(jnp.int32)

        q_t, k_t, v_t, cosine, sine = project(x_in, cache_len, ln_attn, w_q, w_k, w_v, head_dim)
        by_slot = lambda c: c.transpose(1, 2, 3, 0).reshape(n_slots, kv_heads, 8, 8, n_batch)
        k_slots, v_slots = by_slot(k_cache), by_slot(v_cache)
        gains = (q_norm.astype(jnp.float32)[:, None], k_norm.astype(jnp.float32)[:, None])
        len_row = cache_len[None, :]
        w_r = w_router.T

        done, resid, own, far = (), [], [], []
        for c in range(CHUNKS):
            if c:
                len_row, own[c - 1] = lax.optimization_barrier((len_row, own[c - 1]))
            k_full, v_full, attn_t = attend(c, CHUNKS, q_t, k_t, v_t, cosine, sine, len_row, *gains, k_slots, v_slots, done)
            done = (k_full, v_full)
            rows = slice(c * n_rows, (c + 1) * n_rows)
            o_proj = lax.dot_general(attn_t.reshape(-1, n_rows), w_o, (((0,), (0,)), ((), ())), preferred_element_type=jnp.float32)
            resid.append(lax.reduce_precision(x_in[rows].astype(jnp.float32) + o_proj, 8, 7))
            h_moe = norm_scale(resid[c], ln_moe).astype(jnp.bfloat16)
            own.append(h_moe)
            h_x = swap(h_moe, 2)
            h_y = swap(h_moe, 4)
            h_d = swap(h_moe, 6)
            far.append((h_x, h_y, h_d))

            if c == 0:
                picks, own[0] = lax.optimization_barrier((topk_idx.T, own[0]))
                t_blocks = [picks, swap(picks, 2), swap(picks, 4), swap(picks, 6)]

        sums = []
        for c in range(CHUNKS):
            h_o, h_far = own[c], far[c]
            if c == 0:
                h_o, own[-1] = lax.optimization_barrier((h_o, own[-1]))
            else:
                h_far, sums[c - 1] = lax.optimization_barrier((h_far, sums[c - 1]))
            s_o, s_x, s_y, s_d = experts(c, [h_o, *h_far], t_blocks, devs, w_r, w_own, w_par)
            sums.append((s_o, s_x, s_y, s_d))
        outs = []
        sent = []
        for c in range(CHUNKS):
            s_o, s_x, s_y, s_d = sums[c]
            d_x = swap(s_d[0], 2)
            d_y = swap(s_d[1], 4)
            u_x = swap(s_x[0], 2)
            u_y = swap(s_y[1], 4)
            sent.append((d_x, d_y, u_x, u_y))
        last = sums[-1][0][0]
        for c in range(CHUNKS):
            s_o, s_x, s_y, s_d = sums[c]
            d_x, d_y, u_x, u_y = sent[c]
            if c < CHUNKS - 1:
                d_x, d_y, last = lax.optimization_barrier((d_x, d_y, last))
                sums[-1] = ((last, sums[-1][0][1]), *sums[-1][1:])
            m_x, m_y = swap(s_x[1] + d_y, 2), swap(s_y[0] + d_x, 4)
            outs += [s_o[0] + u_x + m_y, s_o[1] + u_y + m_x]
        x_out = (jnp.concatenate(resid, axis=0) + jnp.concatenate(outs, axis=0)).astype(jnp.bfloat16)
        by_row = lambda c: c.reshape(n_slots, kv_heads, head_dim, n_batch).transpose(3, 0, 1, 2)
        return x_out, by_row(k_full), by_row(v_full)

    return jax.shard_map(device_step, mesh=mesh, in_specs=in_specs, out_specs=out_specs, check_vma=False)
```

```python
import functools

import jax
import jax.numpy as jnp
from jax import lax
from jax.experimental import pallas as pl
from jax.experimental.layout import Layout, with_layout_constraint
from jax.experimental.pallas import tpu as pltpu
from jax.sharding import PartitionSpec as P


ROPE_BASE = 1000000.0
NORM_EPS = 1e-6
PIECE = 128
SORTED = 640
ROOM = 768
CHUNKS = 2


def norm_scale(values, gain_vec):
    return values * lax.rsqrt(jnp.mean(values * values, axis=-1, keepdims=True) + NORM_EPS) * gain_vec.astype(jnp.float32)


def attend_kernel(len_ref, cos_ref, sin_ref, qn_ref, kn_ref, q_ref, k_ref, v_ref, kc_ref, vc_ref, ko_ref, vo_ref, o_ref, part_ref, p_ref):
    n_rep = q_ref.shape[0]
    n_slots = kc_ref.shape[0]
    n_batch = q_ref.shape[2]
    unroll = 16

    def norm_rope(values, gain, cosine, sine):
        ms = jnp.mean(values * values, axis=0, keepdims=True)
        values = values * lax.rsqrt(ms + NORM_EPS) * gain
        half = values.shape[0] // 2
        lo, hi = values[:half], values[half:]
        return jnp.concatenate([lo * cosine - hi * sine, hi * cosine + lo * sine], axis=0).astype(jnp.bfloat16)

    for bt in range(n_batch // 128):
        lanes = pl.ds(bt * 128, 128)
        cosine, sine = cos_ref[:, lanes], sin_ref[:, lanes]
        lens = len_ref[:, lanes]
        left0 = jnp.broadcast_to(lens.astype(jnp.float32), (8, 128)).astype(jnp.bfloat16)
        k_new = norm_rope(k_ref[0, :, lanes], kn_ref[...], cosine, sine).reshape(8, 8, 128)
        v_new = v_ref[0, :, lanes].reshape(8, 8, 128)
        qs = [norm_rope(q_ref[r, :, lanes], qn_ref[...], cosine, sine).astype(jnp.float32).reshape(8, 8, 128) for r in range(n_rep)]

        def k_step(i, left):
            for u in range(unroll):
                s = i * unroll + u
                here = left == 0
                sums = [None] * n_rep
                for t in range(8):
                    tile = jnp.where(here, k_new[t], kc_ref[s, 0, t, :, lanes])
                    ko_ref[s, 0, t, :, lanes] = tile
                    wide = tile.astype(jnp.float32)
                    for v in range(1):
                        for r in range(n_rep):
                            term = wide[8 * v:8 * v + 8] * qs[r][1 * t + v]
                            sums[r] = term if sums[r] is None else sums[r] + term
                for r in range(n_rep):
                    part_ref[r, pl.ds(pl.multiple_of(s * 8, 8), 8), :] = sums[r]
                left = left - jnp.ones_like(left)
            return left

        lax.fori_loop(0, n_slots // unroll, k_step, left0)
        seen = lax.broadcasted_iota(jnp.int32, (n_slots, 128), 0) <= lens
        for r in range(n_rep):
            scores = part_ref[r, pl.ds(0, n_slots, stride=8), :]
            for sub in range(1, 8):
                scores = scores + part_ref[r, pl.ds(sub, n_slots, stride=8), :]
            scores = jnp.where(seen, scores * (q_ref.shape[1] ** -0.5), -1e30)
            expd = jnp.exp(scores - jnp.max(scores, axis=0, keepdims=True))
            prob = expd / jnp.sum(expd, axis=0, keepdims=True)
            p_ref[r] = prob.astype(jnp.bfloat16).astype(jnp.float32)

        def v_step(i, carry):
            left, accs = carry
            for u in range(unroll):
                s = i * unroll + u
                here = left == 0
                probs = [jnp.broadcast_to(p_ref[r, pl.ds(s, 1), :], (8, 128)) for r in range(n_rep)]
                accs = list(accs)
                for t in range(8):
                    tile = jnp.where(here, v_new[t], vc_ref[s, 0, t, :, lanes])
                    vo_ref[s, 0, t, :, lanes] = tile
                    wide = tile.astype(jnp.float32)
                    for v in range(1):
                        for r in range(n_rep):
                            at = 8 * r + 1 * t + v
                            accs[at] = accs[at] + wide[8 * v:8 * v + 8] * probs[r]
                accs = tuple(accs)
                left = left - jnp.ones_like(left)
            return left, accs

        zero = jnp.zeros((8, 128), jnp.float32)
        _, accs = lax.fori_loop(0, n_slots // unroll, v_step, (left0, (zero,) * (8 * n_rep)))
        for r in range(n_rep):
            o_ref[r, :, lanes] = jnp.concatenate(accs[8 * r:8 * r + 8], axis=0).astype(jnp.bfloat16)


def project(x_in, cache_len, ln_attn, w_q, w_k, w_v, head_dim):
    n_batch = x_in.shape[0]
    normed = lax.optimization_barrier(norm_scale(x_in.astype(jnp.float32), ln_attn).astype(jnp.bfloat16))

    def proj(w):
        out = with_layout_constraint(jnp.dot(normed, w, preferred_element_type=jnp.float32), Layout(major_to_minor=(1, 0)))
        return out.T.reshape(-1, head_dim, n_batch)

    freq = ROPE_BASE ** (-jnp.arange(head_dim // 2, dtype=jnp.float32) * 2.0 / head_dim)
    angles = freq[:, None] * cache_len.astype(jnp.float32)[None, :]
    return proj(w_q), proj(w_k), proj(w_v).astype(jnp.bfloat16), jnp.cos(angles), jnp.sin(angles)


def attend(chunk, n_chunks, q_t, k_t, v_t, cosine, sine, len_row, q_gain, k_gain, k_cache, v_cache, done):
    n_slots, kv_heads, _, _, n_all = k_cache.shape
    head_dim = q_t.shape[1]
    n_batch = n_all // n_chunks
    n_rep = q_t.shape[0] // kv_heads
    full = lambda *shape: pl.BlockSpec(shape, lambda g: (0,) * len(shape))
    lane = lambda n: pl.BlockSpec((n, n_batch), lambda g: (0, chunk))
    cache_spec = pl.BlockSpec((n_slots, 1, 8, 8, n_batch), lambda g: (0, g, 0, 0, chunk))
    head_spec = lambda n: pl.BlockSpec((n, head_dim, n_batch), lambda g: (g, 0, chunk))
    out_spec = pl.BlockSpec((n_rep, head_dim, n_batch), lambda g: (g, 0, 0))
    cache_shape = jax.ShapeDtypeStruct(k_cache.shape, jnp.bfloat16)
    n_done = len(done)

    def body(*refs):
        attend_kernel(*refs[n_done:])

    return pl.pallas_call(
        body,
        grid=(kv_heads,),
        in_specs=[pl.BlockSpec(memory_space=pl.ANY)] * n_done + [lane(1), lane(head_dim // 2), lane(head_dim // 2), full(head_dim, 1), full(head_dim, 1),
                  head_spec(n_rep), head_spec(1), head_spec(1), cache_spec, cache_spec],
        out_specs=[cache_spec, cache_spec, out_spec],
        out_shape=[cache_shape, cache_shape, jax.ShapeDtypeStruct((q_t.shape[0], head_dim, n_batch), jnp.bfloat16)],
        input_output_aliases={i: i for i in range(n_done)},
        scratch_shapes=[pltpu.VMEM((n_rep, n_slots * 8, 128), jnp.float32), pltpu.VMEM((n_rep, n_slots, 128), jnp.float32)],
        compiler_params=pltpu.CompilerParams(dimension_semantics=("arbitrary",), vmem_limit_bytes=40 * 2**20),
        cost_estimate=pl.CostEstimate(flops=30_000_000_000, bytes_accessed=70_000_000, transcendentals=0),
        name="attend",
    )(*done, len_row, cosine, sine, q_gain, k_gain, q_t, k_t, v_t, k_cache, v_cache)


def expert_kernel(n_sub, e_local, dev_ref, wr_ref, *refs):
    t_refs = refs[:2 * n_sub]
    h_refs = refs[2 * n_sub:4 * n_sub]
    w_refs = refs[4 * n_sub:4 * n_sub + 6]
    o_refs = refs[4 * n_sub + 6:8 * n_sub + 6]
    xs_ref, ys_ref, wg_ref, wu_ref, wd_ref, prow_ref, r_ref, number_ref, number_smem, sem, number_sem = refs[8 * n_sub + 6:]
    bufs = (wg_ref, wu_ref, wd_ref)
    ring = wg_ref.shape[0]
    step = pl.program_id(0)
    steps = 2 * e_local
    src = step // e_local
    half, hidden = h_refs[0].shape

    def copy(e, k, first):
        source = w_refs[k].at[e] if first else w_refs[3 + k].at[e - e_local]
        return pltpu.make_async_copy(source, bufs[k].at[lax.rem(e, ring)], sem.at[lax.rem(e, ring), k])

    def fetch(e):
        for first in (True, False):
            @pl.when((e < e_local) if first else ((e >= e_local) & (e < steps)))
            def _(first=first):
                for k in range(3):
                    copy(e, k, first).start()

    @pl.when(step == 0)
    def _():
        for e in range(ring - 1):
            fetch(jnp.int32(e))
        ys_ref[...] = jnp.zeros_like(ys_ref)
        for j in range(n_sub):
            xs_ref[j, SORTED:, :] = jnp.zeros((ROOM - SORTED, hidden), jnp.bfloat16)

        locals_of = {}
        for q in range(2 * n_sub):
            picks = t_refs[q][...]
            n_experts = wr_ref.shape[0]
            logits = lax.dot_general(wr_ref[...], h_refs[q][...], (((1,), (1,)), ((), ())), preferred_element_type=jnp.float32)
            expert = lax.broadcasted_iota(jnp.int32, (n_experts, half), 0)
            times = jnp.zeros((n_experts, half), jnp.float32)
            for k in range(picks.shape[0]):
                times = times + jnp.where(expert == picks[k:k + 1], 1.0, 0.0)
            chosen = times > 0.0
            top = jnp.max(jnp.where(chosen, logits, -3.4e38), axis=0, keepdims=True)
            expd = jnp.where(chosen, jnp.exp(jnp.where(chosen, logits - top, 0.0)), 0.0)
            gate = expd / jnp.sum(expd, axis=0, keepdims=True)
            for which in range(2):
                low = dev_ref[which] * e_local
                r_ref[2 * q + which:2 * q + which + 1, :] = jnp.sum(jnp.where((expert >= low) & (expert < low + e_local), gate, 0.0), axis=0, keepdims=True)
                here = (picks >= low) & (picks < low + e_local)
                locals_of[q, which] = jnp.sum(jnp.where(here, (picks - low).astype(jnp.float32), 0.0), axis=0, keepdims=True)
        lane_a = lax.broadcasted_iota(jnp.int32, (2 * half, 2 * half), 0)
        lane_b = lax.broadcasted_iota(jnp.int32, (2 * half, 2 * half), 1)
        before = jnp.where(lane_a < lane_b, 1.0, 0.0).astype(jnp.bfloat16)
        local = lax.broadcasted_iota(jnp.int32, (16, 2 * half), 0).astype(jnp.float32)
        for j in range(n_sub):
            for which in range(2):
                loc = jnp.concatenate([locals_of[2 * j, which], locals_of[2 * j + 1, which]], axis=1)
                hot = jnp.where(local == loc, 1.0, 0.0)
                rank = jnp.dot(hot.astype(jnp.bfloat16), before, preferred_element_type=jnp.float32)
                number = jnp.sum(hot, axis=1, keepdims=True)
                padded = ((number.astype(jnp.int32) + 15) // 16 * 16).astype(jnp.float32)
                first = jnp.zeros((1, 1), jnp.float32)
                seat = jnp.zeros((1, 2 * half), jnp.float32)
                for e in range(e_local):
                    seat = seat + hot[e:e + 1] * (rank[e:e + 1] + first)
                    first = first + padded[e:e + 1]
                prow_ref[2 * j + which:2 * j + which + 1, :] = seat.astype(jnp.int32)
                number_ref[2 * j + which] = jnp.broadcast_to(number[:8], (8, 128)).astype(jnp.int32)

    fetch(step + ring - 1)

    @pl.when(step % e_local == 0)
    def _():
        for j in range(n_sub):
            prow = prow_ref[pl.ds(2 * j + src, 1), :]
            for c in range(SORTED // PIECE):
                seat = lax.broadcasted_iota(jnp.int32, (PIECE, 2 * half), 0) + c * PIECE
                hot = jnp.where(seat == prow, 1.0, 0.0).astype(jnp.bfloat16)
                rows = jnp.dot(hot[:, :half], h_refs[2 * j][...], preferred_element_type=jnp.float32)
                rows = rows + jnp.dot(hot[:, half:], h_refs[2 * j + 1][...], preferred_element_type=jnp.float32)
                xs_ref[j, c * PIECE:(c + 1) * PIECE, :] = rows.astype(jnp.bfloat16)

    @pl.when(step == 0)
    def _():
        to_scalars = pltpu.make_async_copy(number_ref, number_smem, number_sem)
        to_scalars.start()
        to_scalars.wait()

    slot = lax.rem(step, ring)
    for k in range(3):
        pltpu.make_async_copy(w_refs[k].at[0], bufs[k].at[slot], sem.at[slot, k]).wait()
    mine_e = step - src * e_local
    counts, starts = [], []
    for j in range(n_sub):
        counts.append((number_smem[2 * j + src, mine_e, 0] + PIECE - 1) // PIECE)
        first = jnp.int32(0)
        for e in range(e_local - 1):
            first = first + jnp.where(e < mine_e, (number_smem[2 * j + src, e, 0] + 15) // 16 * 16, 0)
        starts.append(first)

    def piece(c, carry):
        offs = [pl.multiple_of(jnp.minimum(starts[j] + c * PIECE, SORTED), 16) for j in range(n_sub)]
        rows = jnp.concatenate([xs_ref[j, pl.ds(offs[j], PIECE), :] for j in range(n_sub)], axis=0)
        gate = jnp.dot(rows, wg_ref[slot], preferred_element_type=jnp.float32)
        up = jnp.dot(rows, wu_ref[slot], preferred_element_type=jnp.float32)
        act = (jax.nn.silu(gate) * up).astype(jnp.bfloat16)
        out = jnp.dot(act, wd_ref[slot], preferred_element_type=jnp.float32).astype(jnp.bfloat16)
        for j in range(n_sub):
            @pl.when(c < counts[j])
            def _(j=j):
                ys_ref[j, pl.ds(offs[j], PIECE), :] = out[j * PIECE:(j + 1) * PIECE]
        return carry

    lax.fori_loop(0, functools.reduce(jnp.maximum, counts), piece, 0)

    def column(row):
        return jnp.broadcast_to(row, (128, row.shape[1])).T

    def back(which):
        for j in range(n_sub):
            seat_col = column(prow_ref[2 * j + which:2 * j + which + 1, :].astype(jnp.float32))
            for i in range(2):
                r_col = column(r_ref[2 * (2 * j + i) + which:2 * (2 * j + i) + which + 1, :])
                for c in range(half // PIECE):
                    at = seat_col[i * half + c * PIECE:i * half + (c + 1) * PIECE]
                    lane = lax.broadcasted_iota(jnp.int32, (PIECE, 128), 1).astype(jnp.float32)
                    hot = jnp.concatenate([jnp.where(at == lane + t * 128.0, 1.0, 0.0).astype(jnp.bfloat16) for t in range(SORTED // 128)], axis=1)
                    r_rows = r_col[c * PIECE:(c + 1) * PIECE]
                    mine = jnp.dot(hot, ys_ref[j, :SORTED, :], preferred_element_type=jnp.float32) * jnp.concatenate([r_rows] * (hidden // 128), axis=1)
                    o_ref = o_refs[4 * j + 2 * i + c]
                    o_ref[...] = mine if which == 0 else o_ref[...] + mine

    @pl.when(step == e_local - 1)
    def _():
        back(0)

    @pl.when(step == steps - 1)
    def _():
        back(1)


def experts(chunk, blocks, t_blocks, devs, w_r, w_own, w_par):
    n_sub = len(blocks) // 2
    half, hidden = blocks[0].shape
    e_local, _, ff = w_own[0].shape
    ring = 4
    once = pl.Buffered(1)
    full = lambda *shape: pl.BlockSpec(shape, lambda e, *_: (0,) * len(shape), pipeline_mode=once)
    out = pl.pallas_call(
        functools.partial(expert_kernel, n_sub, e_local),
        grid_spec=pltpu.PrefetchScalarGridSpec(
            num_scalar_prefetch=1,
            grid=(2 * e_local,),
            in_specs=[full(*w_r.shape)] + [pl.BlockSpec((t_blocks[0].shape[0], half), lambda e, *_: (0, chunk))] * (2 * n_sub) + [full(half, hidden)] * (2 * n_sub)
            + [pl.BlockSpec(memory_space=pl.ANY)] * 6,
            out_specs=[full(PIECE, hidden)] * (4 * n_sub),
            scratch_shapes=[pltpu.VMEM((n_sub, ROOM, hidden), jnp.bfloat16)] * 2
            + [pltpu.VMEM((ring, hidden, ff), jnp.bfloat16)] * 2 + [pltpu.VMEM((ring, ff, hidden), jnp.bfloat16)]
            + [pltpu.VMEM((2 * n_sub, 2 * half), jnp.int32), pltpu.VMEM((4 * n_sub, half), jnp.float32), pltpu.VMEM((2 * n_sub, 8, 128), jnp.int32),
               pltpu.SMEM((2 * n_sub, 8, 128), jnp.int32), pltpu.SemaphoreType.DMA((ring, 3)), pltpu.SemaphoreType.DMA],
        ),
        out_shape=[jax.ShapeDtypeStruct((PIECE, hidden), jnp.float32)] * (4 * n_sub),
        compiler_params=pltpu.CompilerParams(dimension_semantics=("arbitrary",), vmem_limit_bytes=58 * 2**20),
        cost_estimate=pl.CostEstimate(flops=n_sub * 16_000_000_000, bytes_accessed=60_000_000, transcendentals=0),
        name="experts",
    )(devs, w_r, *t_blocks, *blocks, *w_own, *w_par)
    return [(out[2 * i], out[2 * i + 1]) for i in range(2 * n_sub)]


def solution(mesh):
    ep_size = mesh.shape['ep']
    row_spec = P(('dp', 'ep'))
    replicated = P()
    expert_spec = P('ep')
    in_specs = (row_spec, row_spec, row_spec, row_spec, row_spec, replicated, replicated, replicated, replicated, replicated, replicated, replicated, replicated, replicated, expert_spec, expert_spec, expert_spec)
    out_specs = (row_spec, row_spec, row_spec)

    def swap(value, bit):
        return lax.ppermute(value, 'ep', [(i, i ^ bit) for i in range(ep_size)])

    def device_step(x_in, k_cache, v_cache, cache_len, topk_idx, ln_attn, w_q, w_k, w_v, q_norm, k_norm, w_o, ln_moe, w_router, w_gate, w_up, w_down):
        me = lax.axis_index('ep')
        n_batch, n_slots, kv_heads, head_dim = k_cache.shape
        n_rows = n_batch // CHUNKS
        w_own = (w_gate, w_up, w_down)
        w_par = tuple(swap(w, 1) for w in w_own)
        devs = jnp.stack([me, me ^ 1]).astype(jnp.int32)

        q_t, k_t, v_t, cosine, sine = project(x_in, cache_len, ln_attn, w_q, w_k, w_v, head_dim)
        by_slot = lambda c: c.transpose(1, 2, 3, 0).reshape(n_slots, kv_heads, 8, 8, n_batch)
        k_slots, v_slots = by_slot(k_cache), by_slot(v_cache)
        gains = (q_norm.astype(jnp.float32)[:, None], k_norm.astype(jnp.float32)[:, None])
        len_row = cache_len[None, :]
        w_r = w_router.T

        done, resid, own, far = (), [], [], []
        for c in range(CHUNKS):
            if c:
                len_row, own[c - 1] = lax.optimization_barrier((len_row, own[c - 1]))
            k_full, v_full, attn_t = attend(c, CHUNKS, q_t, k_t, v_t, cosine, sine, len_row, *gains, k_slots, v_slots, done)
            done = (k_full, v_full)
            rows = slice(c * n_rows, (c + 1) * n_rows)
            o_proj = lax.dot_general(attn_t.reshape(-1, n_rows), w_o, (((0,), (0,)), ((), ())), preferred_element_type=jnp.float32)
            resid.append(lax.reduce_precision(x_in[rows].astype(jnp.float32) + o_proj, 8, 7))
            h_moe = norm_scale(resid[c], ln_moe).astype(jnp.bfloat16)
            own.append(h_moe)
            h_x = swap(h_moe, 2)
            h_y = swap(h_moe, 4)
            h_d = swap(h_moe, 6)
            far.append((h_x, h_y, h_d))

            if c == 0:
                picks, own[0] = lax.optimization_barrier((topk_idx.T, own[0]))
                t_blocks = [picks, swap(picks, 2), swap(picks, 4), swap(picks, 6)]

        def sums_of(c, names):
            ids = ["oxyd".index(n) for n in names]
            blocks = [(own[c], *far[c])[i] for i in ids]
            return experts(c, blocks, [t_blocks[i] for i in ids], devs, w_r, w_own, w_par)

        outs = []
        waiting = None
        for c in range(CHUNKS):
            if c == 0:
                far[0], own[-1] = lax.optimization_barrier((far[0], own[-1]))
            else:
                far[c], s_x = lax.optimization_barrier((far[c], s_x))
                waiting[1] = s_x
            if c:
                s_y, s_d = sums_of(c, "yd")
            else:
                s_o, s_x, s_y, s_d = sums_of(c, "oxyd")
            if c:
                p_o, p_x, p_y, d_x, d_y, u_x, u_y = waiting
                d_x, d_y, s_y = lax.optimization_barrier((d_x, d_y, s_y))
                m_x, m_y = swap(p_x[1] + d_y, 2), swap(p_y[0] + d_x, 4)
                outs += [p_o[0] + u_x + m_y, p_o[1] + u_y + m_x]
            d_x, d_y = swap(s_d[0], 2), swap(s_d[1], 4)
            u_y = swap(s_y[1], 4)
            if c:
                own[c], s_y = lax.optimization_barrier((own[c], s_y))
                s_o, s_x = sums_of(c, "ox")
            u_x = swap(s_x[0], 2)
            waiting = [s_o, s_x, s_y, d_x, d_y, u_x, u_y]
        m_x, m_y = swap(s_x[1] + d_y, 2), swap(s_y[0] + d_x, 4)
        outs += [s_o[0] + u_x + m_y, s_o[1] + u_y + m_x]
        x_out = (jnp.concatenate(resid, axis=0) + jnp.concatenate(outs, axis=0)).astype(jnp.bfloat16)
        by_row = lambda c: c.reshape(n_slots, kv_heads, head_dim, n_batch).transpose(3, 0, 1, 2)
        return x_out, by_row(k_full), by_row(v_full)

    return jax.shard_map(device_step, mesh=mesh, in_specs=in_specs, out_specs=out_specs, check_vma=False)
```
